256 devices in a mesh: rows: 32 (over x, z), cols: 8 (over y, core).
Axes of the slice: x: 4, y: 4, z: 8, core: 2. Of those that a mesh axis runs over, the one named last changes fastest.
Arguments:
- cube: float32 [1, 12288, 12288], P(None, 'rows', 'cols'), may hold values from -480 to 480
Outputs:
- scale_one: float32 [1, 12288, 12288], P(None, 'rows', 'cols')
- scale_two: float32 [1, 12288, 12288], P(None, 'rows', 'cols')
- scale_three: float32 [1, 12288, 12288], P(None, 'rows', 'cols')
- smooth: float32 [1, 12288, 12288], P(None, 'rows', 'cols')
- sigmas: float32 [3, 1], replicated
The draws below stay inside these ranges and needn't reach their ends.
All inputs are finite; a program needn't handle non-finite values.
Results may differ from the reference program's by a relative error of at most 0.0002.
Values sent between devices are 32-bit elements; how exact they have to be, the bound alone decides.
A program may use at most 64 MiB of HBM per device.

```python
import math
import jax
import jax.numpy as jnp
from jax import lax

F = 1
NR = 12288
NC = 12288
LEVELS = 3


def profile(key, count):
    amp_key, phase_key = jax.random.split(key, 2)
    position = jnp.arange(count, dtype=jnp.float32) / (count - 1)
    freqs = jnp.array([1.0, 2.0, 3.0, 5.0, 7.0], jnp.float32)
    amps = jax.random.uniform(amp_key, (5,), jnp.float32, 0.3, 1.0)
    phases = jax.random.uniform(phase_key, (5,), jnp.float32, 0.0, 6.2831853)
    wave = jnp.sum(amps[:, None] * jnp.sin(6.2831853 * freqs[:, None] * position[None, :] + phases[:, None]), axis=0)
    wave = wave / jnp.sum(amps)
    return jnp.exp(math.log(3.0) * (0.5 * position + 0.25 * (1.0 + wave)))


def draw_cube(key, part):
    keys = jax.random.split(jax.random.fold_in(key, 11), 10)
    shape = (F, NR, NC)
    envelope = (profile(keys[4], NR)[:, None] * profile(keys[5], NC)[None, :])[None]
    block_env = (profile(keys[6], NR)[:, None] * profile(keys[7], NC)[None, :])[None]
    rough = jax.random.uniform(keys[1], shape, jnp.float32, 0.5, 1.5)
    channel = jnp.exp(jax.random.uniform(keys[2], (F, 1, 1), jnp.float32, math.log(0.5), math.log(2.0)))
    block_gain = jnp.exp(jax.random.uniform(keys[8], (F, 1, 1), jnp.float32, math.log(0.5), math.log(2.0)))
    coarse = jax.random.truncated_normal(keys[9], -4.0, 4.0, (F, NR // 4, NC // 4), jnp.float32)
    coarse = jnp.repeat(jnp.repeat(coarse, 4, axis=1), 4, axis=2)
    blocky = 0.7 * coarse * block_env * block_gain
    noise = jax.random.truncated_normal(keys[0], -4.0, 4.0, shape, jnp.float32)
    return noise * rough * envelope * channel + blocky


def setup_inputs(seed: int = 0) -> dict:
    key_of = jax.random.split(jax.random.key(seed), 2)
    cube = draw_cube(jax.random.fold_in(key_of[1], 71), 0)
    return {"cube": cube}


def filter_dim(x, dim, step):
    length = x.shape[dim]

    def part(lower, upper):
        return lax.slice_in_dim(x, lower, length - upper, axis=dim)
    outer = (part(0, 4 * step) + part(4 * step, 0)) * 0.0625
    inner = (part(step, 3 * step) + part(3 * step, step)) * 0.25
    return outer + inner + part(2 * step, 2 * step) * 0.375

def reference(cube):
    current = cube
    planes = []
    count = NR * NC
    sigma_rows = []
    for level in range(LEVELS):
        step = 2 ** level
        width = 2 * step
        padded = jnp.pad(current, ((0, 0), (width, width), (width, width)), mode='reflect')
        nextsmooth = filter_dim(filter_dim(padded, 1, step), 2, step)
        plane = current - nextsmooth
        planes.append(plane)
        squares = lax.optimization_barrier(jnp.sum(plane * plane, axis=(1, 2)))
        sigma_rows.append(jnp.sqrt(squares / count + 1e-06))
        current = nextsmooth
    return (planes[0], planes[1], planes[2], current, jnp.stack(sigma_rows))
```

```python
import functools

import jax
import jax.numpy as jnp
from jax import lax
from jax.experimental import pallas as pl
from jax.experimental.pallas import tpu as pltpu
from jax.sharding import PartitionSpec as P

MESH = pl.DeviceIdType.MESH
F32 = jnp.float32

NROW, NCOL = 32, 8
NX, NZ = 4, 8
R, C = 384, 1536
NCH = C // 128
HALO = NCH
OFF = 24
TOP, BOT = OFF, OFF + R
ROWS = R + 2 * OFF
EDGE = 16
PIXELS = float(NROW * NCOL * R * C)


def row_pass(src, c, r, h):
    def at(k):
        return src[c, pl.ds(r + k, 8), :]

    return (at(-2 * h) + at(2 * h)) + (at(-h) + at(h)) * 4.0 + at(0) * 6.0


def stage(src, dst, shift, h, first, last, outs, plane=None, plane_chunks=()):
    lane = lax.broadcasted_iota(jnp.int32, (8, 128), 1)
    lo1, lo2 = lane < h, lane < 2 * h
    hi1, hi2 = lane >= 128 - h, lane >= 128 - 2 * h
    needed = []
    for c in outs:
        for k in ((c - 1) % (NCH + 1), c, (c + 1) % (NCH + 1)):
            if k not in needed:
                needed.append(k)

    def block(i, acc):
        r = pl.multiple_of(first + 8 * i, 8)
        v, rolled = {}, {}
        for c in needed:
            v[c] = row_pass(src, c, r, h)

        def roll(c, s):
            if (c, s) not in rolled:
                rolled[c, s] = pltpu.roll(v[c], s % 128, 1)
            return rolled[c, s]

        for c in outs:
            p, n = (c - 1) % (NCH + 1), (c + 1) % (NCH + 1)
            left1 = jnp.where(lo1, roll(p, h), roll(c, h))
            right1 = jnp.where(hi1, roll(n, -h), roll(c, -h))
            left2 = jnp.where(lo2, roll(p, 2 * h), roll(c, 2 * h))
            right2 = jnp.where(hi2, roll(n, -2 * h), roll(c, -2 * h))
            out = (
                (left2 + right2) * (1.0 / 256)
                + (left1 + right1) * (4.0 / 256)
                + v[c] * (6.0 / 256)
            )
            if shift == 0 or c in plane_chunks:
                dst[c, pl.ds(pl.multiple_of(r - shift, 8), 8), :] = out
            if c in plane_chunks:
                w = src[c, pl.ds(r, 8), :] - out
                plane[c, pl.ds(pl.multiple_of(r - OFF, 8), 8), :] = w
                acc = acc + w * w
        return acc

    return lax.fori_loop(0, (last - first) // 8, block, jnp.zeros((8, 128), F32))


def kernel_main(
    cube, w1, w2, w3, smooth, sigma,
    c0, c1, c2, from_left, from_right, mine, mine2, plane_sums, line_sums,
    load_sem, send_sem, recv_sem, sum_send, sum_recv,
):
    row, col = lax.axis_index("rows"), lax.axis_index("cols")
    x, z = row // NZ, row % NZ
    up, down = row > 0, row < NROW - 1
    left, right = col > 0, col < NCOL - 1
    me_plane = x * NCOL + col

    def both(a, b):
        return jnp.logical_and(a, b)

    everything = pl.ds(0, NCH)
    top_own, bottom_own = pl.ds(TOP, EDGE), pl.ds(BOT - EDGE, EDGE)
    above, below = pl.ds(TOP - EDGE, EDGE), pl.ds(BOT, EDGE)
    own = pl.ds(TOP, R)
    halos = [
        (left, 0, -1, c0.at[0, own], from_right.at[own]),
        (right, 0, 1, c0.at[NCH - 1, own], from_left.at[own]),
        (up, -1, 0, c0.at[everything, top_own], c0.at[everything, below]),
        (down, 1, 0, c0.at[everything, bottom_own], c0.at[everything, above]),
        (both(up, left), -1, -1, c0.at[0, top_own], from_right.at[below]),
        (both(up, right), -1, 1, c0.at[NCH - 1, top_own], from_left.at[below]),
        (both(down, left), 1, -1, c0.at[0, bottom_own], from_right.at[above]),
        (both(down, right), 1, 1, c0.at[NCH - 1, bottom_own], from_left.at[above]),
    ]

    def halo_copy(k):
        _, dr, dc, src, dst = halos[k]
        return pltpu.make_async_remote_copy(
            src_ref=src, dst_ref=dst, send_sem=send_sem.at[k], recv_sem=recv_sem.at[k],
            device_id=(row + dr, col + dc), device_id_type=MESH,
        )

    def load(c, part):
        a, n = ((0, EDGE), (R - EDGE, EDGE), (EDGE, R - 2 * EDGE))[part]
        return pltpu.make_async_copy(
            cube.at[0, pl.ds(a, n), pl.ds(c * 128, 128)],
            c0.at[c, pl.ds(TOP + a, n)],
            load_sem.at[c, part],
        )

    order = [0, NCH - 1] + list(range(1, NCH - 1))
    for c in order:
        load(c, 0).start()
        load(c, 1).start()
    for c in order:
        load(c, 2).start()

    barrier = pltpu.get_barrier_semaphore()
    count = jnp.int32(NX * NCOL - 1 + NZ - 1)
    for exists, dr, dc, _, _ in halos:
        count = count + exists.astype(jnp.int32)

        @pl.when(exists)
        def _():
            pl.semaphore_signal(barrier, inc=1, device_id=(row + dr, col + dc), device_id_type=MESH)

    def plane_peer(k):
        other = (me_plane + k) % (NX * NCOL)
        return ((other // NCOL) * NZ + z, other % NCOL)

    def line_peer(k):
        return (x * NZ + (z + k) % NZ, col)

    for k in range(1, NX * NCOL):
        pl.semaphore_signal(barrier, inc=1, device_id=plane_peer(k), device_id_type=MESH)
    for k in range(1, NZ):
        pl.semaphore_signal(barrier, inc=1, device_id=line_peer(k), device_id_type=MESH)

    for c in order:
        load(c, 0).wait()
        load(c, 1).wait()
    load(0, 2).wait()
    load(NCH - 1, 2).wait()
    pl.semaphore_wait(barrier, count)
    for k in range(8):
        @pl.when(halos[k][0])
        def _():
            halo_copy(k).start()
    for c in order[2:]:
        load(c, 2).wait()

    inner = tuple(range(1, NCH - 1))
    whole = tuple(range(NCH))
    rim = (NCH - 1, HALO, 0)
    rim_own = (NCH - 1, 0)

    a1 = stage(c0, c1, 0, 1, TOP + 8, BOT - 8, whole, w1, inner)
    a2 = stage(c1, c2, 0, 2, TOP + 16, BOT - 16, whole, w2, inner)
    a3 = stage(c2, smooth, OFF, 4, TOP + 24, BOT - 24, inner, w3, inner)

    for k in range(8):
        _, dr, dc, _, _ = halos[k]
        arrives = {0: right, 1: left, 2: down, 3: up,
                   4: both(down, right), 5: both(down, left),
                   6: both(up, right), 7: both(up, left)}[k]

        @pl.when(arrives)
        def _():
            halo_copy(k).wait_recv()

    lane = lax.broadcasted_iota(jnp.int32, (8, 128), 1)
    src_lane = lax.broadcasted_iota(jnp.int32, (128, 128), 0)
    dst_lane = lax.broadcasted_iota(jnp.int32, (128, 128), 1)

    def mirrored(chunk, total, dst):
        turn = (src_lane + dst_lane == total).astype(F32)
        dst[pl.ds(8, ROWS - 16), :] = lax.dot_general(
            c0[chunk, pl.ds(8, ROWS - 16), :], turn, (((1,), (0,)), ((), ())),
            precision=lax.Precision.HIGHEST, preferred_element_type=F32,
        )

    @pl.when(jnp.logical_not(left))
    def _():
        mirrored(0, 128, from_left)

    @pl.when(jnp.logical_not(right))
    def _():
        mirrored(NCH - 1, 126, from_right)

    def merge(i, carry):
        r = pl.multiple_of(8 + 8 * i, 8)
        c0[HALO, pl.ds(r, 8), :] = jnp.where(
            lane < 64, from_right[pl.ds(r, 8), :], from_left[pl.ds(r, 8), :]
        )
        return carry

    lax.fori_loop(0, (ROWS - 16) // 8, merge, 0)

    @pl.when(jnp.logical_not(up))
    def _():
        for i in range(1, 15):
            c0[:, pl.ds(TOP - i, 1), :] = c0[:, pl.ds(TOP + i, 1), :]

    @pl.when(jnp.logical_not(down))
    def _():
        for i in range(1, 15):
            c0[:, pl.ds(BOT - 1 + i, 1), :] = c0[:, pl.ds(BOT - 1 - i, 1), :]

    every = tuple(range(NCH + 1))
    a1 += stage(c0, c1, 0, 1, TOP + 8, BOT - 8, rim, w1, rim_own)
    a2 += stage(c1, c2, 0, 2, TOP + 16, BOT - 16, rim, w2, rim_own)
    a3 += stage(c2, smooth, OFF, 4, TOP + 24, BOT - 24, rim_own, w3, rim_own)
    stage(c0, c1, 0, 1, TOP - 16, TOP, every)
    stage(c0, c1, 0, 1, BOT, BOT + 16, every)
    a1 += stage(c0, c1, 0, 1, TOP, TOP + 8, every, w1, whole)
    a1 += stage(c0, c1, 0, 1, BOT - 8, BOT, every, w1, whole)
    stage(c1, c2, 0, 2, TOP - 8, TOP, every)
    stage(c1, c2, 0, 2, BOT, BOT + 8, every)
    a2 += stage(c1, c2, 0, 2, TOP, TOP + 16, every, w2, whole)
    a2 += stage(c1, c2, 0, 2, BOT - 16, BOT, every, w2, whole)
    a3 += stage(c2, smooth, OFF, 4, TOP, TOP + 24, whole, w3, whole)
    a3 += stage(c2, smooth, OFF, 4, BOT - 24, BOT, whole, w3, whole)

    lane1 = lax.broadcasted_iota(jnp.int32, (1, 128), 1)

    def total(a):
        return jnp.sum(jnp.sum(a, axis=0, keepdims=True), axis=1, keepdims=True)

    vec = jnp.where(lane1 == 0, total(a1), jnp.where(lane1 == 1, total(a2), total(a3)))

    def gather(value, own_ref, slots, index, count, peer, which):
        own_ref[...] = value
        slots[pl.ds(index, 1)] = value[None]
        for k in range(1, count):
            pltpu.make_async_remote_copy(
                src_ref=own_ref, dst_ref=slots.at[index],
                send_sem=sum_send.at[which], recv_sem=sum_recv.at[which],
                device_id=peer(k), device_id_type=MESH,
            ).start()
        arrived = slots.at[pl.ds(0, count - 1)]
        pltpu.make_async_copy(arrived, arrived, sum_recv.at[which]).wait()
        return jnp.sum(slots[...], axis=0)

    vec = gather(vec, mine, plane_sums, me_plane, NX * NCOL, plane_peer, 0)
    vec = gather(vec, mine2, line_sums, z, NZ, line_peer, 1)
    sigma[...] = jnp.sqrt(vec * (1.0 / PIXELS) + 1e-6)

    for which, slots, count in ((0, plane_sums, NX * NCOL), (1, line_sums, NZ)):
        sent = slots.at[pl.ds(0, count - 1)]
        pltpu.make_async_copy(sent, sent, sum_send.at[which]).wait()
    for k in range(8):
        @pl.when(halos[k][0])
        def _():
            halo_copy(k).wait_send()


def kernel_write(w1, w2, w3, smooth, sigma, o1, o2, o3, o4, o5, sem):
    pairs = ((w1, o1), (w2, o2), (w3, o3), (smooth, o4))
    for i, (a, o) in enumerate(pairs):
        for c in range(NCH):
            pltpu.make_async_copy(
                a.at[c], o.at[0, :, pl.ds(c * 128, 128)], sem.at[i]
            ).start()
    o5[...] = sigma[:, :3]
    for i, (a, o) in enumerate(pairs):
        pltpu.make_async_copy(a, a, sem.at[i]).wait()


def on_device(cube):
    vmem = pl.BlockSpec(memory_space=pltpu.VMEM)
    hbm = pl.BlockSpec(memory_space=pltpu.HBM)
    block = jax.ShapeDtypeStruct((NCH, R, 128), F32)
    cube = pltpu.with_memory_space_constraint(cube, pltpu.HBM)
    planes = pl.pallas_call(
        kernel_main,
        out_shape=[block] * 4 + [jax.ShapeDtypeStruct((1, 128), F32)],
        in_specs=[hbm],
        out_specs=[vmem] * 5,
        scratch_shapes=[
            pltpu.VMEM((NCH + 1, ROWS, 128), F32),
            pltpu.VMEM((NCH + 1, ROWS, 128), F32),
            pltpu.VMEM((NCH + 1, ROWS, 128), F32),
            pltpu.VMEM((ROWS, 128), F32),
            pltpu.VMEM((ROWS, 128), F32),
            pltpu.VMEM((1, 128), F32),
            pltpu.VMEM((1, 128), F32),
            pltpu.VMEM((NX * NCOL, 1, 128), F32),
            pltpu.VMEM((NZ, 1, 128), F32),
            pltpu.SemaphoreType.DMA((NCH, 3)),
            pltpu.SemaphoreType.DMA((8,)),
            pltpu.SemaphoreType.DMA((8,)),
            pltpu.SemaphoreType.DMA((2,)),
            pltpu.SemaphoreType.DMA((2,)),
        ],
        compiler_params=pltpu.CompilerParams(
            collective_id=0, has_side_effects=True, vmem_limit_bytes=40 * 2**20
        ),
        name="starlet",
    )(cube)
    out = jax.ShapeDtypeStruct((1, R, C), F32)
    o = pl.pallas_call(
        kernel_write,
        out_shape=[out] * 4 + [jax.ShapeDtypeStruct((1, 3), F32)],
        in_specs=[vmem] * 5,
        out_specs=[hbm] * 4 + [vmem],
        scratch_shapes=[pltpu.SemaphoreType.DMA((4,))],
        compiler_params=pltpu.CompilerParams(vmem_limit_bytes=16 * 2**20),
        name="write",
    )(*planes)
    return o[0], o[1], o[2], o[3], o[4].T


def solution(mesh):
    block = P(None, "rows", "cols")
    return jax.shard_map(
        on_device,
        mesh=mesh,
        in_specs=(block,),
        out_specs=(block,) * 4 + (P(),),
        check_vma=False,
    )
```

```python
import functools

import jax
import jax.numpy as jnp
from jax import lax
from jax.experimental import pallas as pl
from jax.experimental.pallas import tpu as pltpu
from jax.sharding import PartitionSpec as P

MESH = pl.DeviceIdType.MESH
F32 = jnp.float32

NROW, NCOL = 32, 8
NX, NZ = 4, 8
R, C = 384, 1536
NCH = C // 128
HALO = NCH
OFF = 24
TOP, BOT = OFF, OFF + R
ROWS = R + 2 * OFF
EDGE = 16
PIXELS = float(NROW * NCOL * R * C)


def row_pass(src, c, r, h):
    def at(k):
        return src[c, pl.ds(r + k, 8), :]

    ends = (at(-2 * h) + at(2 * h)) * (1.0 / 256)
    return ends + (at(-h) + at(h)) * (4.0 / 256) + at(0) * (6.0 / 256)


def stage(src, dst, shift, h, rows, outs, plane=None, plane_chunks=()):
    lane = lax.broadcasted_iota(jnp.int32, (8, 128), 1)
    lo1, lo2 = lane < h, lane < 2 * h
    hi1, hi2 = lane >= 128 - h, lane >= 128 - 2 * h
    ring = NCH + 1
    needed = list(dict.fromkeys(k for c in outs for k in ((c - 1) % ring, c, (c + 1) % ring)))

    def block(r, inside, acc):
        v, rolled = {}, {}
        for c in needed:
            v[c] = row_pass(src, c, r, h)

        def roll(c, s):
            if (c, s) not in rolled:
                rolled[c, s] = pltpu.roll(v[c], s % 128, 1)
            return rolled[c, s]

        for c in outs:
            p, n = (c - 1) % ring, (c + 1) % ring
            left1 = jnp.where(lo1, roll(p, h), roll(c, h))
            right1 = jnp.where(hi1, roll(n, -h), roll(c, -h))
            left2 = jnp.where(lo2, roll(p, 2 * h), roll(c, 2 * h))
            right2 = jnp.where(hi2, roll(n, -2 * h), roll(c, -2 * h))
            out = (left2 + right2) + (left1 + right1) * 4.0 + v[c] * 6.0
            if shift == 0 or c in plane_chunks:
                dst[c, pl.ds(r - shift, 8), :] = out
            if inside and c in plane_chunks:
                w = src[c, pl.ds(r, 8), :] - out
                plane[c, pl.ds(r - OFF, 8), :] = w
                acc = acc + w * w
        return acc

    acc = jnp.zeros((8, 128), F32)
    if isinstance(rows, list):
        for r in rows:
            acc = block(r, TOP <= r < BOT, acc)
        return acc
    n = len(rows)
    u = next(q for q in (6, 4, 3, 2, 1) if n % q == 0)

    def several(i, acc):
        for j in range(u):
            acc = block(pl.multiple_of(rows[0] + 8 * (i * u + j), 8), True, acc)
        return acc

    return lax.fori_loop(0, n // u, several, acc)


def kernel_main(
    cube, w1, w2, w3, smooth, sigma,
    c0, c1, c2, from_left, from_right, mine, mine2, plane_sums, line_sums,
    load_sem, send_sem, recv_sem, sum_send, sum_recv,
):
    row, col = lax.axis_index("rows"), lax.axis_index("cols")
    x, z = row // NZ, row % NZ
    up, down = row > 0, row < NROW - 1
    left, right = col > 0, col < NCOL - 1
    me_plane = x * NCOL + col

    def both(a, b):
        return jnp.logical_and(a, b)

    everything = pl.ds(0, NCH)
    top_own, bottom_own = pl.ds(TOP, EDGE), pl.ds(BOT - EDGE, EDGE)
    above, below = pl.ds(TOP - EDGE, EDGE), pl.ds(BOT, EDGE)
    own = pl.ds(TOP, R)
    halos = [
        (left, 0, -1, c0.at[0, own], from_right.at[own]),
        (right, 0, 1, c0.at[NCH - 1, own], from_left.at[own]),
        (up, -1, 0, c0.at[everything, top_own], c0.at[everything, below]),
        (down, 1, 0, c0.at[everything, bottom_own], c0.at[everything, above]),
        (both(up, left), -1, -1, c0.at[0, top_own], from_right.at[below]),
        (both(up, right), -1, 1, c0.at[NCH - 1, top_own], from_left.at[below]),
        (both(down, left), 1, -1, c0.at[0, bottom_own], from_right.at[above]),
        (both(down, right), 1, 1, c0.at[NCH - 1, bottom_own], from_left.at[above]),
    ]

    def halo_copy(k):
        _, dr, dc, src, dst = halos[k]
        return pltpu.make_async_remote_copy(
            src_ref=src, dst_ref=dst, send_sem=send_sem.at[k], recv_sem=recv_sem.at[k],
            device_id=(row + dr, col + dc), device_id_type=MESH,
        )

    def load(c, part):
        a, n = ((0, EDGE), (R - EDGE, EDGE), (EDGE, R - 2 * EDGE))[part]
        return pltpu.make_async_copy(
            cube.at[0, pl.ds(a, n), pl.ds(c * 128, 128)],
            c0.at[c, pl.ds(TOP + a, n)],
            load_sem.at[c, part],
        )

    order = [0, NCH - 1] + list(range(1, NCH - 1))
    for c in order:
        load(c, 0).start()
        load(c, 1).start()
    for c in order:
        load(c, 2).start()

    barrier = pltpu.get_barrier_semaphore()
    count = jnp.int32(NX * NCOL - 1 + NZ - 1)
    for exists, dr, dc, _, _ in halos:
        count = count + exists.astype(jnp.int32)

        @pl.when(exists)
        def _():
            pl.semaphore_signal(barrier, inc=1, device_id=(row + dr, col + dc), device_id_type=MESH)

    def plane_peer(k):
        other = (me_plane + k) % (NX * NCOL)
        return ((other // NCOL) * NZ + z, other % NCOL)

    def line_peer(k):
        return (x * NZ + (z + k) % NZ, col)

    for k in range(1, NX * NCOL):
        pl.semaphore_signal(barrier, inc=1, device_id=plane_peer(k), device_id_type=MESH)
    for k in range(1, NZ):
        pl.semaphore_signal(barrier, inc=1, device_id=line_peer(k), device_id_type=MESH)

    for c in order:
        load(c, 0).wait()
        load(c, 1).wait()
    load(0, 2).wait()
    load(NCH - 1, 2).wait()
    pl.semaphore_wait(barrier, count)
    for k in range(8):
        @pl.when(halos[k][0])
        def _():
            halo_copy(k).start()
    for c in order[2:]:
        load(c, 2).wait()

    inner = tuple(range(1, NCH - 1))
    whole = tuple(range(NCH))
    rim = (NCH - 1, HALO, 0)
    rim_own = (NCH - 1, 0)

    mid1, mid2, mid3 = (range(TOP + k, BOT - k, 8) for k in (8, 16, 24))
    a1 = stage(c0, c1, 0, 1, mid1, whole, w1, inner)
    a2 = stage(c1, c2, 0, 2, mid2, whole, w2, inner)
    a3 = stage(c2, smooth, OFF, 4, mid3, inner, w3, inner)

    for k in range(8):
        _, dr, dc, _, _ = halos[k]
        arrives = {0: right, 1: left, 2: down, 3: up,
                   4: both(down, right), 5: both(down, left),
                   6: both(up, right), 7: both(up, left)}[k]

        @pl.when(arrives)
        def _():
            halo_copy(k).wait_recv()

    lane = lax.broadcasted_iota(jnp.int32, (8, 128), 1)
    src_lane = lax.broadcasted_iota(jnp.int32, (128, 128), 0)
    dst_lane = lax.broadcasted_iota(jnp.int32, (128, 128), 1)

    def mirrored(chunk, total, dst):
        turn = (src_lane + dst_lane == total).astype(F32)
        dst[pl.ds(8, ROWS - 16), :] = lax.dot_general(
            c0[chunk, pl.ds(8, ROWS - 16), :], turn, (((1,), (0,)), ((), ())),
            precision=lax.Precision.HIGHEST, preferred_element_type=F32,
        )

    @pl.when(jnp.logical_not(left))
    def _():
        mirrored(0, 128, from_left)

    @pl.when(jnp.logical_not(right))
    def _():
        mirrored(NCH - 1, 126, from_right)

    def merge(i, carry):
        r = pl.multiple_of(8 + 8 * i, 8)
        c0[HALO, pl.ds(r, 8), :] = jnp.where(
            lane < 64, from_right[pl.ds(r, 8), :], from_left[pl.ds(r, 8), :]
        )
        return carry

    lax.fori_loop(0, (ROWS - 16) // 8, merge, 0)

    @pl.when(jnp.logical_not(up))
    def _():
        for i in range(1, 15):
            c0[:, pl.ds(TOP - i, 1), :] = c0[:, pl.ds(TOP + i, 1), :]

    @pl.when(jnp.logical_not(down))
    def _():
        for i in range(1, 15):
            c0[:, pl.ds(BOT - 1 + i, 1), :] = c0[:, pl.ds(BOT - 1 - i, 1), :]

    every = tuple(range(NCH + 1))
    a1 += stage(c0, c1, 0, 1, mid1, rim, w1, rim_own)
    a2 += stage(c1, c2, 0, 2, mid2, rim, w2, rim_own)
    a3 += stage(c2, smooth, OFF, 4, mid3, rim_own, w3, rim_own)

    def ends(a, b):
        return list(range(TOP + a, TOP + b, 8)) + list(range(BOT - b, BOT - a, 8))

    a1 += stage(c0, c1, 0, 1, ends(-16, 8), every, w1, whole)
    a2 += stage(c1, c2, 0, 2, ends(-8, 16), every, w2, whole)
    a3 += stage(c2, smooth, OFF, 4, ends(0, 24), whole, w3, whole)

    lane1 = lax.broadcasted_iota(jnp.int32, (1, 128), 1)

    def total(a):
        return jnp.sum(jnp.sum(a, axis=0, keepdims=True), axis=1, keepdims=True)

    vec = jnp.where(lane1 == 0, total(a1), jnp.where(lane1 == 1, total(a2), total(a3)))

    def gather(value, own_ref, slots, index, count, peer, which):
        own_ref[...] = value
        slots[pl.ds(index, 1)] = value[None]
        for k in range(1, count):
            pltpu.make_async_remote_copy(
                src_ref=own_ref, dst_ref=slots.at[index],
                send_sem=sum_send.at[which], recv_sem=sum_recv.at[which],
                device_id=peer(k), device_id_type=MESH,
            ).start()
        arrived = slots.at[pl.ds(0, count - 1)]
        pltpu.make_async_copy(arrived, arrived, sum_recv.at[which]).wait()
        return jnp.sum(slots[...], axis=0)

    vec = gather(vec, mine, plane_sums, me_plane, NX * NCOL, plane_peer, 0)
    vec = gather(vec, mine2, line_sums, z, NZ, line_peer, 1)
    sigma[...] = jnp.sqrt(vec * (1.0 / PIXELS) + 1e-6)

    for which, slots, count in ((0, plane_sums, NX * NCOL), (1, line_sums, NZ)):
        sent = slots.at[pl.ds(0, count - 1)]
        pltpu.make_async_copy(sent, sent, sum_send.at[which]).wait()
    for k in range(8):
        @pl.when(halos[k][0])
        def _():
            halo_copy(k).wait_send()


def kernel_write(w1, w2, w3, smooth, sigma, o1, o2, o3, o4, o5, sem):
    pairs = ((w1, o1), (w2, o2), (w3, o3), (smooth, o4))
    for i, (a, o) in enumerate(pairs):
        for c in range(NCH):
            pltpu.make_async_copy(
                a.at[c], o.at[0, :, pl.ds(c * 128, 128)], sem.at[i]
            ).start()
    o5[...] = sigma[:, :3]
    for i, (a, o) in enumerate(pairs):
        pltpu.make_async_copy(a, a, sem.at[i]).wait()


def on_device(cube):
    vmem = pl.BlockSpec(memory_space=pltpu.VMEM)
    hbm = pl.BlockSpec(memory_space=pltpu.HBM)
    block = jax.ShapeDtypeStruct((NCH, R, 128), F32)
    cube = pltpu.with_memory_space_constraint(cube, pltpu.HBM)
    planes = pl.pallas_call(
        kernel_main,
        out_shape=[block] * 4 + [jax.ShapeDtypeStruct((1, 128), F32)],
        in_specs=[hbm],
        out_specs=[vmem] * 5,
        scratch_shapes=[
            pltpu.VMEM((NCH + 1, ROWS, 128), F32),
            pltpu.VMEM((NCH + 1, ROWS, 128), F32),
            pltpu.VMEM((NCH + 1, ROWS, 128), F32),
            pltpu.VMEM((ROWS, 128), F32),
            pltpu.VMEM((ROWS, 128), F32),
            pltpu.VMEM((1, 128), F32),
            pltpu.VMEM((1, 128), F32),
            pltpu.VMEM((NX * NCOL, 1, 128), F32),
            pltpu.VMEM((NZ, 1, 128), F32),
            pltpu.SemaphoreType.DMA((NCH, 3)),
            pltpu.SemaphoreType.DMA((8,)),
            pltpu.SemaphoreType.DMA((8,)),
            pltpu.SemaphoreType.DMA((2,)),
            pltpu.SemaphoreType.DMA((2,)),
        ],
        compiler_params=pltpu.CompilerParams(
            collective_id=0, has_side_effects=True, vmem_limit_bytes=40 * 2**20
        ),
        name="starlet",
    )(cube)
    out = jax.ShapeDtypeStruct((1, R, C), F32)
    o = pl.pallas_call(
        kernel_write,
        out_shape=[out] * 4 + [jax.ShapeDtypeStruct((1, 3), F32)],
        in_specs=[vmem] * 5,
        out_specs=[hbm] * 4 + [vmem],
        scratch_shapes=[pltpu.SemaphoreType.DMA((4,))],
        compiler_params=pltpu.CompilerParams(vmem_limit_bytes=16 * 2**20),
        name="write",
    )(*planes)
    return o[0], o[1], o[2], o[3], o[4].T


def solution(mesh):
    block = P(None, "rows", "cols")
    return jax.shard_map(
        on_device,
        mesh=mesh,
        in_specs=(block,),
        out_specs=(block,) * 4 + (P(),),
        check_vma=False,
    )
```

```python
import functools

import jax
import jax.numpy as jnp
from jax import lax
from jax.experimental import pallas as pl
from jax.experimental.pallas import tpu as pltpu
from jax.sharding import PartitionSpec as P

MESH = pl.DeviceIdType.MESH
F32 = jnp.float32

NROW, NCOL = 32, 8
NX, NZ = 4, 8
R, C = 384, 1536
NCH = C // 128
HALO = NCH
OFF = 24
TOP, BOT = OFF, OFF + R
ROWS = R + 2 * OFF
EDGE = 16
UNROLL = 6
PIXELS = float(NROW * NCOL * R * C)


def row_pass(src, c, r, h):
    def at(k):
        return src[c, pl.ds(r + k, 8), :]

    ends = (at(-2 * h) + at(2 * h)) * (1.0 / 256)
    return ends + (at(-h) + at(h)) * (4.0 / 256) + at(0) * (6.0 / 256)


def stage(src, dst, shift, h, rows, outs, plane=None, plane_chunks=()):
    lane = lax.broadcasted_iota(jnp.int32, (8, 128), 1)
    lo1, lo2 = lane < h, lane < 2 * h
    hi1, hi2 = lane >= 128 - h, lane >= 128 - 2 * h
    ring = NCH + 1
    needed = list(dict.fromkeys(k for c in outs for k in ((c - 1) % ring, c, (c + 1) % ring)))

    def block(r, inside, acc):
        v, rolled = {}, {}
        for c in needed:
            v[c] = row_pass(src, c, r, h)

        def roll(c, s):
            if (c, s) not in rolled:
                rolled[c, s] = pltpu.roll(v[c], s % 128, 1)
            return rolled[c, s]

        for c in outs:
            p, n = (c - 1) % ring, (c + 1) % ring
            left1 = jnp.where(lo1, roll(p, h), roll(c, h))
            right1 = jnp.where(hi1, roll(n, -h), roll(c, -h))
            left2 = jnp.where(lo2, roll(p, 2 * h), roll(c, 2 * h))
            right2 = jnp.where(hi2, roll(n, -2 * h), roll(c, -2 * h))
            out = (left2 + right2) + (left1 + right1) * 4.0 + v[c] * 6.0
            if shift == 0 or c in plane_chunks:
                dst[c, pl.ds(r - shift, 8), :] = out
            if inside and c in plane_chunks:
                w = src[c, pl.ds(r, 8), :] - out
                plane[c, pl.ds(r - OFF, 8), :] = w
                acc = acc + w * w
        return acc

    acc = jnp.zeros((8, 128), F32)
    if isinstance(rows, list):
        for r in rows:
            acc = block(r, TOP <= r < BOT, acc)
        return acc
    n = len(rows)

    def several(i, acc):
        for j in range(UNROLL):
            acc = block(pl.multiple_of(rows[0] + 8 * (i * UNROLL + j), 8), True, acc)
        return acc

    acc = lax.fori_loop(0, n // UNROLL, several, acc)
    for r in rows[n - n % UNROLL:]:
        acc = block(r, True, acc)
    return acc


def kernel_main(
    cube, w1, w2, w3, smooth, sigma,
    c0, c1, c2, from_left, from_right, mine, mine2, plane_sums, line_sums,
    load_sem, send_sem, recv_sem, sum_send, sum_recv,
):
    row, col = lax.axis_index("rows"), lax.axis_index("cols")
    x, z = row // NZ, row % NZ
    up, down = row > 0, row < NROW - 1
    left, right = col > 0, col < NCOL - 1
    me_plane = x * NCOL + col

    def both(a, b):
        return jnp.logical_and(a, b)

    everything = pl.ds(0, NCH)
    top_own, bottom_own = pl.ds(TOP, EDGE), pl.ds(BOT - EDGE, EDGE)
    above, below = pl.ds(TOP - EDGE, EDGE), pl.ds(BOT, EDGE)
    own = pl.ds(TOP, R)
    halos = [
        (left, 0, -1, c0.at[0, own], from_right.at[own]),
        (right, 0, 1, c0.at[NCH - 1, own], from_left.at[own]),
        (up, -1, 0, c0.at[everything, top_own], c0.at[everything, below]),
        (down, 1, 0, c0.at[everything, bottom_own], c0.at[everything, above]),
        (both(up, left), -1, -1, c0.at[0, top_own], from_right.at[below]),
        (both(up, right), -1, 1, c0.at[NCH - 1, top_own], from_left.at[below]),
        (both(down, left), 1, -1, c0.at[0, bottom_own], from_right.at[above]),
        (both(down, right), 1, 1, c0.at[NCH - 1, bottom_own], from_left.at[above]),
    ]

    def halo_copy(k):
        _, dr, dc, src, dst = halos[k]
        return pltpu.make_async_remote_copy(
            src_ref=src, dst_ref=dst, send_sem=send_sem.at[k], recv_sem=recv_sem.at[k],
            device_id=(row + dr, col + dc), device_id_type=MESH,
        )

    def load(c, part):
        a, n = ((0, EDGE), (R - EDGE, EDGE), (EDGE, R - 2 * EDGE))[part]
        return pltpu.make_async_copy(
            cube.at[0, pl.ds(a, n), pl.ds(c * 128, 128)],
            c0.at[c, pl.ds(TOP + a, n)],
            load_sem.at[c, part],
        )

    order = [0, NCH - 1] + list(range(1, NCH - 1))
    for c in order:
        load(c, 0).start()
        load(c, 1).start()
    for c in order:
        load(c, 2).start()

    barrier = pltpu.get_barrier_semaphore()
    count = jnp.int32(NX * NCOL - 1 + NZ - 1)
    for exists, dr, dc, _, _ in halos:
        count = count + exists.astype(jnp.int32)

        @pl.when(exists)
        def _():
            pl.semaphore_signal(barrier, inc=1, device_id=(row + dr, col + dc), device_id_type=MESH)

    def plane_peer(k):
        other = (me_plane + k) % (NX * NCOL)
        return ((other // NCOL) * NZ + z, other % NCOL)

    def line_peer(k):
        return (x * NZ + (z + k) % NZ, col)

    for k in range(1, NX * NCOL):
        pl.semaphore_signal(barrier, inc=1, device_id=plane_peer(k), device_id_type=MESH)
    for k in range(1, NZ):
        pl.semaphore_signal(barrier, inc=1, device_id=line_peer(k), device_id_type=MESH)

    for c in order:
        load(c, 0).wait()
        load(c, 1).wait()
    load(0, 2).wait()
    load(NCH - 1, 2).wait()
    pl.semaphore_wait(barrier, count)
    for k in range(8):
        @pl.when(halos[k][0])
        def _():
            halo_copy(k).start()
    for c in order[2:]:
        load(c, 2).wait()

    inner = tuple(range(1, NCH - 1))
    whole = tuple(range(NCH))
    rim = (NCH - 1, HALO, 0)
    rim_own = (NCH - 1, 0)

    every = tuple(range(NCH + 1))
    mid1, mid2, mid3 = (range(TOP + k, BOT - k, 8) for k in (8, 16, 24))

    arrives = (right, left, down, up,
               both(down, right), both(down, left), both(up, right), both(up, left))

    def wait_halo(k):
        @pl.when(arrives[k])
        def _():
            halo_copy(k).wait_recv()

    src_lane = lax.broadcasted_iota(jnp.int32, (128, 128), 0)
    dst_lane = lax.broadcasted_iota(jnp.int32, (128, 128), 1)

    def halo_chunk(spans):
        def mirrored(chunk, total, dst):
            turn = (src_lane + dst_lane == total).astype(F32)
            for span in spans:
                dst[span, :] = lax.dot_general(
                    c0[chunk, span, :], turn, (((1,), (0,)), ((), ())),
                    precision=lax.Precision.HIGHEST, preferred_element_type=F32,
                )

        @pl.when(jnp.logical_not(left))
        def _():
            mirrored(0, 128, from_left)

        @pl.when(jnp.logical_not(right))
        def _():
            mirrored(NCH - 1, 126, from_right)

        for span in spans:
            c0[HALO, span, :] = jnp.where(
                lax.broadcasted_iota(jnp.int32, (span.size, 128), 1) < 64,
                from_right[span, :], from_left[span, :],
            )

    a1 = stage(c0, c1, 0, 1, mid1, inner, w1, inner)
    wait_halo(0)
    wait_halo(1)
    halo_chunk([own])
    a1 += stage(c0, c1, 0, 1, mid1, rim, w1, rim_own)
    a2 = stage(c1, c2, 0, 2, mid2, every, w2, whole)
    a3 = stage(c2, smooth, OFF, 4, mid3, whole, w3, whole)

    for k in range(2, 8):
        wait_halo(k)
    halo_chunk([above, below])

    @pl.when(jnp.logical_not(up))
    def _():
        for i in range(1, 15):
            c0[:, pl.ds(TOP - i, 1), :] = c0[:, pl.ds(TOP + i, 1), :]

    @pl.when(jnp.logical_not(down))
    def _():
        for i in range(1, 15):
            c0[:, pl.ds(BOT - 1 + i, 1), :] = c0[:, pl.ds(BOT - 1 - i, 1), :]

    def ends(a, b):
        return list(range(TOP + a, TOP + b, 8)) + list(range(BOT - b, BOT - a, 8))

    a1 += stage(c0, c1, 0, 1, ends(-16, 8), every, w1, whole)
    a2 += stage(c1, c2, 0, 2, ends(-8, 16), every, w2, whole)
    a3 += stage(c2, smooth, OFF, 4, ends(0, 24), whole, w3, whole)

    lane1 = lax.broadcasted_iota(jnp.int32, (1, 128), 1)

    def total(a):
        return jnp.sum(jnp.sum(a, axis=0, keepdims=True), axis=1, keepdims=True)

    vec = jnp.where(lane1 == 0, total(a1), jnp.where(lane1 == 1, total(a2), total(a3)))

    def gather(value, own_ref, slots, index, count, peer, which):
        own_ref[...] = value
        slots[pl.ds(index, 1)] = value[None]
        for k in range(1, count):
            pltpu.make_async_remote_copy(
                src_ref=own_ref, dst_ref=slots.at[index],
                send_sem=sum_send.at[which], recv_sem=sum_recv.at[which],
                device_id=peer(k), device_id_type=MESH,
            ).start()
        arrived = slots.at[pl.ds(0, count - 1)]
        pltpu.make_async_copy(arrived, arrived, sum_recv.at[which]).wait()
        return jnp.sum(slots[...], axis=0)

    vec = gather(vec, mine, plane_sums, me_plane, NX * NCOL, plane_peer, 0)
    vec = gather(vec, mine2, line_sums, z, NZ, line_peer, 1)
    sigma[...] = jnp.sqrt(vec * (1.0 / PIXELS) + 1e-6)

    for which, slots, count in ((0, plane_sums, NX * NCOL), (1, line_sums, NZ)):
        sent = slots.at[pl.ds(0, count - 1)]
        pltpu.make_async_copy(sent, sent, sum_send.at[which]).wait()
    for k in range(8):
        @pl.when(halos[k][0])
        def _():
            halo_copy(k).wait_send()


def kernel_write(w1, w2, w3, smooth, sigma, o1, o2, o3, o4, o5, sem):
    pairs = ((w1, o1), (w2, o2), (w3, o3), (smooth, o4))
    for i, (a, o) in enumerate(pairs):
        for c in range(NCH):
            pltpu.make_async_copy(
                a.at[c], o.at[0, :, pl.ds(c * 128, 128)], sem.at[i]
            ).start()
    o5[...] = sigma[:, :3]
    for i, (a, o) in enumerate(pairs):
        pltpu.make_async_copy(a, a, sem.at[i]).wait()


def on_device(cube):
    vmem = pl.BlockSpec(memory_space=pltpu.VMEM)
    hbm = pl.BlockSpec(memory_space=pltpu.HBM)
    block = jax.ShapeDtypeStruct((NCH, R, 128), F32)
    cube = pltpu.with_memory_space_constraint(cube, pltpu.HBM)
    planes = pl.pallas_call(
        kernel_main,
        out_shape=[block] * 4 + [jax.ShapeDtypeStruct((1, 128), F32)],
        in_specs=[hbm],
        out_specs=[vmem] * 5,
        scratch_shapes=[
            pltpu.VMEM((NCH + 1, ROWS, 128), F32),
            pltpu.VMEM((NCH + 1, ROWS, 128), F32),
            pltpu.VMEM((NCH + 1, ROWS, 128), F32),
            pltpu.VMEM((ROWS, 128), F32),
            pltpu.VMEM((ROWS, 128), F32),
            pltpu.VMEM((1, 128), F32),
            pltpu.VMEM((1, 128), F32),
            pltpu.VMEM((NX * NCOL, 1, 128), F32),
            pltpu.VMEM((NZ, 1, 128), F32),
            pltpu.SemaphoreType.DMA((NCH, 3)),
            pltpu.SemaphoreType.DMA((8,)),
            pltpu.SemaphoreType.DMA((8,)),
            pltpu.SemaphoreType.DMA((2,)),
            pltpu.SemaphoreType.DMA((2,)),
        ],
        compiler_params=pltpu.CompilerParams(
            collective_id=0, has_side_effects=True, vmem_limit_bytes=40 * 2**20
        ),
        name="starlet",
    )(cube)
    out = jax.ShapeDtypeStruct((1, R, C), F32)
    o = pl.pallas_call(
        kernel_write,
        out_shape=[out] * 4 + [jax.ShapeDtypeStruct((1, 3), F32)],
        in_specs=[vmem] * 5,
        out_specs=[hbm] * 4 + [vmem],
        scratch_shapes=[pltpu.SemaphoreType.DMA((4,))],
        compiler_params=pltpu.CompilerParams(vmem_limit_bytes=16 * 2**20),
        name="write",
    )(*planes)
    return o[0], o[1], o[2], o[3], o[4].T


def solution(mesh):
    block = P(None, "rows", "cols")
    return jax.shard_map(
        on_device,
        mesh=mesh,
        in_specs=(block,),
        out_specs=(block,) * 4 + (P(),),
        check_vma=False,
    )
```

```python
import functools

import jax
import jax.numpy as jnp
from jax import lax
from jax.experimental import pallas as pl
from jax.experimental.pallas import tpu as pltpu
from jax.sharding import PartitionSpec as P

MESH = pl.DeviceIdType.MESH
F32 = jnp.float32

NROW, NCOL = 32, 8
NX, NZ = 4, 8
R, C = 384, 1536
NCH = C // 128
HALO = NCH
OFF = 24
TOP, BOT = OFF, OFF + R
ROWS = R + 2 * OFF
EDGE = 16
UNROLL = 6
PIXELS = float(NROW * NCOL * R * C)


def row_pass(src, c, r, h):
    def at(k):
        return src[c, pl.ds(r + k, 8), :]

    ends = (at(-2 * h) + at(2 * h)) * (1.0 / 256)
    return ends + (at(-h) + at(h)) * (4.0 / 256) + at(0) * (6.0 / 256)


def stage(src, dst, shift, h, rows, outs, plane=None, plane_chunks=()):
    lane = lax.broadcasted_iota(jnp.int32, (8, 128), 1)
    lo1, lo2 = lane < h, lane < 2 * h
    hi1, hi2 = lane >= 128 - h, lane >= 128 - 2 * h
    ring = NCH + 1
    needed = list(dict.fromkeys(k for c in outs for k in ((c - 1) % ring, c, (c + 1) % ring)))

    def block(r, inside, acc):
        v, rolled = {}, {}
        for c in needed:
            v[c] = row_pass(src, c, r, h)

        def roll(c, s):
            if (c, s) not in rolled:
                rolled[c, s] = pltpu.roll(v[c], s % 128, 1)
            return rolled[c, s]

        for c in outs:
            p, n = (c - 1) % ring, (c + 1) % ring
            left1 = jnp.where(lo1, roll(p, h), roll(c, h))
            right1 = jnp.where(hi1, roll(n, -h), roll(c, -h))
            left2 = jnp.where(lo2, roll(p, 2 * h), roll(c, 2 * h))
            right2 = jnp.where(hi2, roll(n, -2 * h), roll(c, -2 * h))
            out = (left2 + right2) + (left1 + right1) * 4.0 + v[c] * 6.0
            if shift == 0 or c in plane_chunks:
                dst[c, pl.ds(r - shift, 8), :] = out
            if inside and c in plane_chunks:
                w = src[c, pl.ds(r, 8), :] - out
                plane[c, pl.ds(r - OFF, 8), :] = w
                acc = acc + w * w
        return acc

    acc = jnp.zeros((8, 128), F32)
    if isinstance(rows, list):
        for r in rows:
            acc = block(r, TOP <= r < BOT, acc)
        return acc
    n = len(rows)

    def several(i, acc):
        for j in range(UNROLL):
            acc = block(pl.multiple_of(rows[0] + 8 * (i * UNROLL + j), 8), True, acc)
        return acc

    acc = lax.fori_loop(0, n // UNROLL, several, acc)
    for r in rows[n - n % UNROLL:]:
        acc = block(r, True, acc)
    return acc


def kernel_main(
    cube, w1, w2, w3, smooth, sigma,
    c0, c1, c2, from_left, from_right, mine, mine2, plane_sums, line_sums,
    load_sem, send_sem, recv_sem, sum_send, sum_recv,
):
    row, col = lax.axis_index("rows"), lax.axis_index("cols")
    x, z = row // NZ, row % NZ
    up, down = row > 0, row < NROW - 1
    left, right = col > 0, col < NCOL - 1
    me_plane = x * NCOL + col

    def both(a, b):
        return jnp.logical_and(a, b)

    everything = pl.ds(0, NCH)
    top_own, bottom_own = pl.ds(TOP, EDGE), pl.ds(BOT - EDGE, EDGE)
    above, below = pl.ds(TOP - EDGE, EDGE), pl.ds(BOT, EDGE)
    own = pl.ds(TOP, R)
    halos = [
        (left, 0, -1, c0.at[0, own], from_right.at[own]),
        (right, 0, 1, c0.at[NCH - 1, own], from_left.at[own]),
        (up, -1, 0, c0.at[everything, top_own], c0.at[everything, below]),
        (down, 1, 0, c0.at[everything, bottom_own], c0.at[everything, above]),
        (both(up, left), -1, -1, c0.at[0, top_own], from_right.at[below]),
        (both(up, right), -1, 1, c0.at[NCH - 1, top_own], from_left.at[below]),
        (both(down, left), 1, -1, c0.at[0, bottom_own], from_right.at[above]),
        (both(down, right), 1, 1, c0.at[NCH - 1, bottom_own], from_left.at[above]),
    ]

    def halo_copy(k):
        _, dr, dc, src, dst = halos[k]
        return pltpu.make_async_remote_copy(
            src_ref=src, dst_ref=dst, send_sem=send_sem.at[k], recv_sem=recv_sem.at[k],
            device_id=(row + dr, col + dc), device_id_type=MESH,
        )

    def load(c, part):
        a, n = ((0, EDGE), (R - EDGE, EDGE), (EDGE, R - 2 * EDGE))[part]
        return pltpu.make_async_copy(
            cube.at[0, pl.ds(a, n), pl.ds(c * 128, 128)],
            c0.at[c, pl.ds(TOP + a, n)],
            load_sem.at[c, part],
        )

    barrier = pltpu.get_barrier_semaphore()
    count = jnp.int32(NX * NCOL - 1 + NZ - 1)
    for exists, dr, dc, _, _ in halos:
        count = count + exists.astype(jnp.int32)

        @pl.when(exists)
        def _():
            pl.semaphore_signal(barrier, inc=1, device_id=(row + dr, col + dc), device_id_type=MESH)

    plane_order = [(dx, dc) for dx in range(NX) for dc in range(NCOL) if dx or dc]
    plane_order.sort(key=lambda p: -(min(p[0], NX - p[0]) + min(p[1] // 2, NCOL // 2 - p[1] // 2)))
    line_order = sorted(range(1, NZ), key=lambda k: -min(k, NZ - k))

    def plane_peer(k):
        dx, dc = k
        return (((x + dx) % NX) * NZ + z, (col + dc) % NCOL)

    def line_peer(k):
        return (x * NZ + (z + k) % NZ, col)

    for k in plane_order:
        pl.semaphore_signal(barrier, inc=1, device_id=plane_peer(k), device_id_type=MESH)
    for k in line_order:
        pl.semaphore_signal(barrier, inc=1, device_id=line_peer(k), device_id_type=MESH)

    order = [0, NCH - 1] + list(range(1, NCH - 1))
    for c in order:
        load(c, 0).start()
        load(c, 1).start()
    for c in order:
        load(c, 2).start()

    for c in order:
        load(c, 0).wait()
        load(c, 1).wait()
    load(0, 2).wait()
    load(NCH - 1, 2).wait()
    pl.semaphore_wait(barrier, count)
    for k in range(8):
        @pl.when(halos[k][0])
        def _():
            halo_copy(k).start()
    for c in order[2:]:
        load(c, 2).wait()

    inner = tuple(range(1, NCH - 1))
    whole = tuple(range(NCH))
    rim = (NCH - 1, HALO, 0)
    rim_own = (NCH - 1, 0)

    every = tuple(range(NCH + 1))
    mid1, mid2, mid3 = (range(TOP + k, BOT - k, 8) for k in (8, 16, 24))

    arrives = (right, left, down, up,
               both(down, right), both(down, left), both(up, right), both(up, left))

    def wait_halo(k):
        @pl.when(arrives[k])
        def _():
            halo_copy(k).wait_recv()

    src_lane = lax.broadcasted_iota(jnp.int32, (128, 128), 0)
    dst_lane = lax.broadcasted_iota(jnp.int32, (128, 128), 1)

    def halo_chunk(spans):
        def mirrored(chunk, total, dst):
            turn = (src_lane + dst_lane == total).astype(F32)
            for span in spans:
                dst[span, :] = lax.dot_general(
                    c0[chunk, span, :], turn, (((1,), (0,)), ((), ())),
                    precision=lax.Precision.HIGHEST, preferred_element_type=F32,
                )

        @pl.when(jnp.logical_not(left))
        def _():
            mirrored(0, 128, from_left)

        @pl.when(jnp.logical_not(right))
        def _():
            mirrored(NCH - 1, 126, from_right)

        for span in spans:
            c0[HALO, span, :] = jnp.where(
                lax.broadcasted_iota(jnp.int32, (span.size, 128), 1) < 64,
                from_right[span, :], from_left[span, :],
            )

    inner2 = tuple(range(2, NCH - 2))
    rim2 = (NCH - 2, NCH - 1, HALO, 0, 1)
    rim2_own = (NCH - 2, NCH - 1, 0, 1)
    a1 = stage(c0, c1, 0, 1, mid1, inner, w1, inner)
    a2 = stage(c1, c2, 0, 2, mid2, inner2, w2, inner2)
    wait_halo(0)
    wait_halo(1)
    halo_chunk([own])
    a1 += stage(c0, c1, 0, 1, mid1, rim, w1, rim_own)
    a2 += stage(c1, c2, 0, 2, mid2, rim2, w2, rim2_own)
    a3 = stage(c2, smooth, OFF, 4, mid3, whole, w3, whole)

    for k in range(2, 8):
        wait_halo(k)
    halo_chunk([above, below])

    @pl.when(jnp.logical_not(up))
    def _():
        for i in range(1, 15):
            c0[:, pl.ds(TOP - i, 1), :] = c0[:, pl.ds(TOP + i, 1), :]

    @pl.when(jnp.logical_not(down))
    def _():
        for i in range(1, 15):
            c0[:, pl.ds(BOT - 1 + i, 1), :] = c0[:, pl.ds(BOT - 1 - i, 1), :]

    def ends(a, b):
        return list(range(TOP + a, TOP + b, 8)) + list(range(BOT - b, BOT - a, 8))

    a1 += stage(c0, c1, 0, 1, ends(-16, 8), every, w1, whole)
    a2 += stage(c1, c2, 0, 2, ends(-8, 16), every, w2, whole)
    a3 += stage(c2, smooth, OFF, 4, ends(0, 24), whole, w3, whole)

    lane1 = lax.broadcasted_iota(jnp.int32, (1, 128), 1)

    def total(a):
        return jnp.sum(jnp.sum(a, axis=0, keepdims=True), axis=1, keepdims=True)

    vec = jnp.where(lane1 == 0, total(a1), jnp.where(lane1 == 1, total(a2), total(a3)))

    def gather(value, own_ref, slots, index, count, peer, steps, which):
        own_ref[...] = value
        slots[pl.ds(index, 1)] = value[None]
        for k in steps:
            pltpu.make_async_remote_copy(
                src_ref=own_ref, dst_ref=slots.at[index],
                send_sem=sum_send.at[which], recv_sem=sum_recv.at[which],
                device_id=peer(k), device_id_type=MESH,
            ).start()
        arrived = slots.at[pl.ds(0, count - 1)]
        pltpu.make_async_copy(arrived, arrived, sum_recv.at[which]).wait()
        return jnp.sum(slots[...], axis=0)

    vec = gather(vec, mine, plane_sums, me_plane, NX * NCOL, plane_peer, plane_order, 0)
    vec = gather(vec, mine2, line_sums, z, NZ, line_peer, line_order, 1)
    sigma[...] = jnp.sqrt(vec * (1.0 / PIXELS) + 1e-6)

    for which, slots, count in ((0, plane_sums, NX * NCOL), (1, line_sums, NZ)):
        sent = slots.at[pl.ds(0, count - 1)]
        pltpu.make_async_copy(sent, sent, sum_send.at[which]).wait()
    for k in range(8):
        @pl.when(halos[k][0])
        def _():
            halo_copy(k).wait_send()


def kernel_write(w1, w2, w3, smooth, sigma, o1, o2, o3, o4, o5, sem):
    pairs = ((w1, o1), (w2, o2), (w3, o3), (smooth, o4))
    for i, (a, o) in enumerate(pairs):
        for c in range(NCH):
            pltpu.make_async_copy(
                a.at[c], o.at[0, :, pl.ds(c * 128, 128)], sem.at[i]
            ).start()
    o5[...] = sigma[:, :3]
    for i, (a, o) in enumerate(pairs):
        pltpu.make_async_copy(a, a, sem.at[i]).wait()


def on_device(cube):
    vmem = pl.BlockSpec(memory_space=pltpu.VMEM)
    hbm = pl.BlockSpec(memory_space=pltpu.HBM)
    block = jax.ShapeDtypeStruct((NCH, R, 128), F32)
    cube = pltpu.with_memory_space_constraint(cube, pltpu.HBM)
    planes = pl.pallas_call(
        kernel_main,
        out_shape=[block] * 4 + [jax.ShapeDtypeStruct((1, 128), F32)],
        in_specs=[hbm],
        out_specs=[vmem] * 5,
        scratch_shapes=[
            pltpu.VMEM((NCH + 1, ROWS, 128), F32),
            pltpu.VMEM((NCH + 1, ROWS, 128), F32),
            pltpu.VMEM((NCH + 1, ROWS, 128), F32),
            pltpu.VMEM((ROWS, 128), F32),
            pltpu.VMEM((ROWS, 128), F32),
            pltpu.VMEM((1, 128), F32),
            pltpu.VMEM((1, 128), F32),
            pltpu.VMEM((NX * NCOL, 1, 128), F32),
            pltpu.VMEM((NZ, 1, 128), F32),
            pltpu.SemaphoreType.DMA((NCH, 3)),
            pltpu.SemaphoreType.DMA((8,)),
            pltpu.SemaphoreType.DMA((8,)),
            pltpu.SemaphoreType.DMA((2,)),
            pltpu.SemaphoreType.DMA((2,)),
        ],
        compiler_params=pltpu.CompilerParams(
            collective_id=0, has_side_effects=True, vmem_limit_bytes=40 * 2**20
        ),
        name="starlet",
    )(cube)
    out = jax.ShapeDtypeStruct((1, R, C), F32)
    o = pl.pallas_call(
        kernel_write,
        out_shape=[out] * 4 + [jax.ShapeDtypeStruct((1, 3), F32)],
        in_specs=[vmem] * 5,
        out_specs=[hbm] * 4 + [vmem],
        scratch_shapes=[pltpu.SemaphoreType.DMA((4,))],
        compiler_params=pltpu.CompilerParams(vmem_limit_bytes=16 * 2**20),
        name="write",
    )(*planes)
    return o[0], o[1], o[2], o[3], o[4].T


def solution(mesh):
    block = P(None, "rows", "cols")
    return jax.shard_map(
        on_device,
        mesh=mesh,
        in_specs=(block,),
        out_specs=(block,) * 4 + (P(),),
        check_vma=False,
    )
```

```python
import functools

import jax
import jax.numpy as jnp
from jax import lax
from jax.experimental import pallas as pl
from jax.experimental.pallas import tpu as pltpu
from jax.sharding import PartitionSpec as P

MESH = pl.DeviceIdType.MESH
F32 = jnp.float32

NROW, NCOL = 32, 8
NX, NZ = 4, 8
R, C = 384, 1536
NCH = C // 128
HALO = NCH
OFF = 24
TOP, BOT = OFF, OFF + R
ROWS = R + 2 * OFF
EDGE = 16
CUT = 8 * ((R // 8 - 2) // 2) + 16
PIXELS = float(NROW * NCOL * R * C)


def row_pass(src, c, r, h):
    def at(k):
        return src[c, pl.ds(r + k, 8), :]

    ends = (at(-2 * h) + at(2 * h)) * (1.0 / 256)
    return ends + (at(-h) + at(h)) * (4.0 / 256) + at(0) * (6.0 / 256)


def stage(src, dst, shift, h, rows, outs, plane=None, plane_chunks=()):
    lane = lax.broadcasted_iota(jnp.int32, (8, 128), 1)
    lo1, lo2 = lane < h, lane < 2 * h
    hi1, hi2 = lane >= 128 - h, lane >= 128 - 2 * h
    ring = NCH + 1
    needed = list(dict.fromkeys(k for c in outs for k in ((c - 1) % ring, c, (c + 1) % ring)))

    def block(r, inside, acc):
        v, rolled = {}, {}
        for c in needed:
            v[c] = row_pass(src, c, r, h)

        def roll(c, s):
            if (c, s) not in rolled:
                rolled[c, s] = pltpu.roll(v[c], s % 128, 1)
            return rolled[c, s]

        for c in outs:
            p, n = (c - 1) % ring, (c + 1) % ring
            left1 = jnp.where(lo1, roll(p, h), roll(c, h))
            right1 = jnp.where(hi1, roll(n, -h), roll(c, -h))
            left2 = jnp.where(lo2, roll(p, 2 * h), roll(c, 2 * h))
            right2 = jnp.where(hi2, roll(n, -2 * h), roll(c, -2 * h))
            out = (left2 + right2) + (left1 + right1) * 4.0 + v[c] * 6.0
            if shift == 0 or c in plane_chunks:
                dst[c, pl.ds(r - shift, 8), :] = out
            if inside and c in plane_chunks:
                w = src[c, pl.ds(r, 8), :] - out
                plane[c, pl.ds(r - OFF, 8), :] = w
                acc = acc + w * w
        return acc

    acc = jnp.zeros((8, 128), F32)
    if isinstance(rows, list):
        for r in rows:
            acc = block(r, TOP <= r < BOT, acc)
        return acc
    n = len(rows)
    u = n // 2 if n % 2 == 0 else n

    def several(i, acc):
        for j in range(u):
            acc = block(pl.multiple_of(rows[0] + 8 * (i * u + j), 8), True, acc)
        return acc

    return lax.fori_loop(0, n // u, several, acc)


def kernel_main(
    cube, w1, w2, w3, smooth, sigma,
    c0, c1, c2, from_left, from_right, mine, mine2, plane_sums, line_sums,
    load_sem, send_sem, recv_sem, sum_send, sum_recv,
):
    row, col = lax.axis_index("rows"), lax.axis_index("cols")
    x, z = row // NZ, row % NZ
    up, down = row > 0, row < NROW - 1
    left, right = col > 0, col < NCOL - 1
    me_plane = x * NCOL + col

    def both(a, b):
        return jnp.logical_and(a, b)

    everything = pl.ds(0, NCH)
    top_own, bottom_own = pl.ds(TOP, EDGE), pl.ds(BOT - EDGE, EDGE)
    above, below = pl.ds(TOP - EDGE, EDGE), pl.ds(BOT, EDGE)
    own = pl.ds(TOP, R)
    halos = [
        (left, 0, -1, c0.at[0, own], from_right.at[own]),
        (right, 0, 1, c0.at[NCH - 1, own], from_left.at[own]),
        (up, -1, 0, c0.at[everything, top_own], c0.at[everything, below]),
        (down, 1, 0, c0.at[everything, bottom_own], c0.at[everything, above]),
        (both(up, left), -1, -1, c0.at[0, top_own], from_right.at[below]),
        (both(up, right), -1, 1, c0.at[NCH - 1, top_own], from_left.at[below]),
        (both(down, left), 1, -1, c0.at[0, bottom_own], from_right.at[above]),
        (both(down, right), 1, 1, c0.at[NCH - 1, bottom_own], from_left.at[above]),
    ]

    def halo_copy(k):
        _, dr, dc, src, dst = halos[k]
        return pltpu.make_async_remote_copy(
            src_ref=src, dst_ref=dst, send_sem=send_sem.at[k], recv_sem=recv_sem.at[k],
            device_id=(row + dr, col + dc), device_id_type=MESH,
        )

    def load(c, part):
        a, n = ((0, EDGE), (R - EDGE, EDGE), (EDGE, CUT - EDGE), (CUT, R - EDGE - CUT))[part]
        return pltpu.make_async_copy(
            cube.at[0, pl.ds(a, n), pl.ds(c * 128, 128)],
            c0.at[c, pl.ds(TOP + a, n)],
            load_sem.at[c, part],
        )

    barrier = pltpu.get_barrier_semaphore()
    count = jnp.int32(NX * NCOL - 1 + NZ - 1)
    for exists, dr, dc, _, _ in halos:
        count = count + exists.astype(jnp.int32)

        @pl.when(exists)
        def _():
            pl.semaphore_signal(barrier, inc=1, device_id=(row + dr, col + dc), device_id_type=MESH)

    plane_order = [(dx, dc) for dx in range(NX) for dc in range(NCOL) if dx or dc]
    plane_order.sort(key=lambda p: -(min(p[0], NX - p[0]) + min(p[1] // 2, NCOL // 2 - p[1] // 2)))
    line_order = sorted(range(1, NZ), key=lambda k: -min(k, NZ - k))

    def plane_peer(k):
        dx, dc = k
        return (((x + dx) % NX) * NZ + z, (col + dc) % NCOL)

    def line_peer(k):
        return (x * NZ + (z + k) % NZ, col)

    for k in plane_order:
        pl.semaphore_signal(barrier, inc=1, device_id=plane_peer(k), device_id_type=MESH)
    for k in line_order:
        pl.semaphore_signal(barrier, inc=1, device_id=line_peer(k), device_id_type=MESH)

    order = [0, NCH - 1] + list(range(1, NCH - 1))
    for c in order:
        load(c, 0).start()
        load(c, 1).start()
    for c in order[:2]:
        load(c, 2).start()
        load(c, 3).start()
    for part in (2, 3):
        for c in order[2:]:
            load(c, part).start()

    for c in order:
        load(c, 0).wait()
        load(c, 1).wait()
    for c in order[:2]:
        load(c, 2).wait()
        load(c, 3).wait()
    pl.semaphore_wait(barrier, count)
    for k in range(8):
        @pl.when(halos[k][0])
        def _():
            halo_copy(k).start()
    inner = tuple(range(1, NCH - 1))
    whole = tuple(range(NCH))
    rim = (NCH - 1, HALO, 0)
    rim_own = (NCH - 1, 0)

    every = tuple(range(NCH + 1))
    mid1, mid2, mid3 = (range(TOP + k, BOT - k, 8) for k in (8, 16, 24))

    arrives = (right, left, down, up,
               both(down, right), both(down, left), both(up, right), both(up, left))

    def wait_halo(k):
        @pl.when(arrives[k])
        def _():
            halo_copy(k).wait_recv()

    src_lane = lax.broadcasted_iota(jnp.int32, (128, 128), 0)
    dst_lane = lax.broadcasted_iota(jnp.int32, (128, 128), 1)

    def halo_chunk(spans):
        def mirrored(chunk, total, dst):
            turn = (src_lane + dst_lane == total).astype(F32)
            for span in spans:
                dst[span, :] = lax.dot_general(
                    c0[chunk, span, :], turn, (((1,), (0,)), ((), ())),
                    precision=lax.Precision.HIGHEST, preferred_element_type=F32,
                )

        @pl.when(jnp.logical_not(left))
        def _():
            mirrored(0, 128, from_left)

        @pl.when(jnp.logical_not(right))
        def _():
            mirrored(NCH - 1, 126, from_right)

        for span in spans:
            c0[HALO, span, :] = jnp.where(
                lax.broadcasted_iota(jnp.int32, (span.size, 128), 1) < 64,
                from_right[span, :], from_left[span, :],
            )

    inner2 = tuple(range(2, NCH - 2))
    rim2 = (NCH - 2, NCH - 1, HALO, 0, 1)
    rim2_own = (NCH - 2, NCH - 1, 0, 1)
    half = len(mid1) // 2
    for c in order[2:]:
        load(c, 2).wait()
    a1 = stage(c0, c1, 0, 1, mid1[:half], inner, w1, inner)
    for c in order[2:]:
        load(c, 3).wait()
    a1 += stage(c0, c1, 0, 1, mid1[half:], inner, w1, inner)
    a2 = stage(c1, c2, 0, 2, mid2, inner2, w2, inner2)
    wait_halo(0)
    wait_halo(1)
    halo_chunk([own])
    a1 += stage(c0, c1, 0, 1, mid1, rim, w1, rim_own)
    a2 += stage(c1, c2, 0, 2, mid2, rim2, w2, rim2_own)
    a3 = stage(c2, smooth, OFF, 4, mid3, whole, w3, whole)

    for k in range(2, 8):
        wait_halo(k)
    halo_chunk([above, below])

    @pl.when(jnp.logical_not(up))
    def _():
        for i in range(1, 15):
            c0[:, pl.ds(TOP - i, 1), :] = c0[:, pl.ds(TOP + i, 1), :]

    @pl.when(jnp.logical_not(down))
    def _():
        for i in range(1, 15):
            c0[:, pl.ds(BOT - 1 + i, 1), :] = c0[:, pl.ds(BOT - 1 - i, 1), :]

    def ends(a, b):
        return list(range(TOP + a, TOP + b, 8)) + list(range(BOT - b, BOT - a, 8))

    a1 += stage(c0, c1, 0, 1, ends(-16, 8), every, w1, whole)
    a2 += stage(c1, c2, 0, 2, ends(-8, 16), every, w2, whole)
    a3 += stage(c2, smooth, OFF, 4, ends(0, 24), whole, w3, whole)

    lane1 = lax.broadcasted_iota(jnp.int32, (1, 128), 1)

    def total(a):
        return jnp.sum(jnp.sum(a, axis=0, keepdims=True), axis=1, keepdims=True)

    vec = jnp.where(lane1 == 0, total(a1), jnp.where(lane1 == 1, total(a2), total(a3)))

    def gather(value, own_ref, slots, index, count, peer, steps, which):
        own_ref[...] = value
        slots[pl.ds(index, 1)] = value[None]
        for k in steps:
            pltpu.make_async_remote_copy(
                src_ref=own_ref, dst_ref=slots.at[index],
                send_sem=sum_send.at[which], recv_sem=sum_recv.at[which],
                device_id=peer(k), device_id_type=MESH,
            ).start()
        arrived = slots.at[pl.ds(0, count - 1)]
        pltpu.make_async_copy(arrived, arrived, sum_recv.at[which]).wait()
        return jnp.sum(slots[...], axis=0)

    vec = gather(vec, mine, plane_sums, me_plane, NX * NCOL, plane_peer, plane_order, 0)
    vec = gather(vec, mine2, line_sums, z, NZ, line_peer, line_order, 1)
    sigma[...] = jnp.sqrt(vec * (1.0 / PIXELS) + 1e-6)

    for which, slots, count in ((0, plane_sums, NX * NCOL), (1, line_sums, NZ)):
        sent = slots.at[pl.ds(0, count - 1)]
        pltpu.make_async_copy(sent, sent, sum_send.at[which]).wait()
    for k in range(8):
        @pl.when(halos[k][0])
        def _():
            halo_copy(k).wait_send()


def kernel_write(w1, w2, w3, smooth, sigma, o1, o2, o3, o4, o5, sem):
    pairs = ((w1, o1), (w2, o2), (w3, o3), (smooth, o4))
    for i, (a, o) in enumerate(pairs):
        for c in range(NCH):
            pltpu.make_async_copy(
                a.at[c], o.at[0, :, pl.ds(c * 128, 128)], sem.at[i]
            ).start()
    o5[...] = sigma[:, :3]
    for i, (a, o) in enumerate(pairs):
        pltpu.make_async_copy(a, a, sem.at[i]).wait()


def on_device(cube):
    vmem = pl.BlockSpec(memory_space=pltpu.VMEM)
    hbm = pl.BlockSpec(memory_space=pltpu.HBM)
    block = jax.ShapeDtypeStruct((NCH, R, 128), F32)
    cube = pltpu.with_memory_space_constraint(cube, pltpu.HBM)
    planes = pl.pallas_call(
        kernel_main,
        out_shape=[block] * 4 + [jax.ShapeDtypeStruct((1, 128), F32)],
        in_specs=[hbm],
        out_specs=[vmem] * 5,
        scratch_shapes=[
            pltpu.VMEM((NCH + 1, ROWS, 128), F32),
            pltpu.VMEM((NCH + 1, ROWS, 128), F32),
            pltpu.VMEM((NCH + 1, ROWS, 128), F32),
            pltpu.VMEM((ROWS, 128), F32),
            pltpu.VMEM((ROWS, 128), F32),
            pltpu.VMEM((1, 128), F32),
            pltpu.VMEM((1, 128), F32),
            pltpu.VMEM((NX * NCOL, 1, 128), F32),
            pltpu.VMEM((NZ, 1, 128), F32),
            pltpu.SemaphoreType.DMA((NCH, 4)),
            pltpu.SemaphoreType.DMA((8,)),
            pltpu.SemaphoreType.DMA((8,)),
            pltpu.SemaphoreType.DMA((2,)),
            pltpu.SemaphoreType.DMA((2,)),
        ],
        compiler_params=pltpu.CompilerParams(
            collective_id=0, has_side_effects=True, vmem_limit_bytes=40 * 2**20
        ),
        name="starlet",
    )(cube)
    out = jax.ShapeDtypeStruct((1, R, C), F32)
    o = pl.pallas_call(
        kernel_write,
        out_shape=[out] * 4 + [jax.ShapeDtypeStruct((1, 3), F32)],
        in_specs=[vmem] * 5,
        out_specs=[hbm] * 4 + [vmem],
        scratch_shapes=[pltpu.SemaphoreType.DMA((4,))],
        compiler_params=pltpu.CompilerParams(vmem_limit_bytes=16 * 2**20),
        name="write",
    )(*planes)
    return o[0], o[1], o[2], o[3], o[4].T


def solution(mesh):
    block = P(None, "rows", "cols")
    return jax.shard_map(
        on_device,
        mesh=mesh,
        in_specs=(block,),
        out_specs=(block,) * 4 + (P(),),
        check_vma=False,
    )
```
